32 devices in a mesh: head: 4 (over x, core), batch: 8 (over z, y).
Axes of the slice: x: 2, y: 2, z: 4, core: 2. Of those that a mesh axis runs over, the one named last changes fastest.
Arguments:
- embedded: bfloat16 [4, 128, 2048], P(None, 'batch'), may hold values from -6 to 6
- states: bfloat16 [128, 32, 128, 128], P('batch', 'head'), may hold values from -6 to 6
- w_query: bfloat16 [2048, 2048], P(None, 'head'), may hold values from -0.125 to 0.125
- w_key: bfloat16 [2048, 2048], P(None, 'head'), may hold values from -0.125 to 0.125
- w_value: bfloat16 [2048, 4096], P(None, 'head'), may hold values from -0.125 to 0.125
- w_output_gate: bfloat16 [2048, 4096], P(None, 'head'), may hold values from -0.125 to 0.125
- w_beta: bfloat16 [2048, 32], P(None, 'head'), may hold values from -0.125 to 0.125
- w_decay: bfloat16 [2048, 32], P(None, 'head'), may hold values from -0.125 to 0.125
- decay_rate: float32 [32], replicated, may hold values from 0.05 to 4
- decay_bias: float32 [32], replicated, may hold values from -3 to 1
- head_gain: float32 [128], replicated, may hold values from 0.5 to 1.5
- input_gain: float32 [2048], replicated, may hold values from 0.5 to 1.5
- w_out: bfloat16 [4096, 2048], P('head'), may hold values from -0.09375 to 0.09375
- final_gain: float32 [2048], replicated, may hold values from 0.5 to 1.5
- lm_head: bfloat16 [2048, 131072], P(None, ('head', 'batch')), may hold values from -1 to 1
- targets: int32 [128, 4], replicated, may hold values from 0 to 131071
- active: int32 [128, 4], replicated, may hold values 0 or 1
Outputs:
- scores: float32 [128, 4], P('batch')
The draws below stay inside these ranges and needn't reach their ends.
All inputs are finite; a program needn't handle non-finite values.
Results may differ from the reference program's by a relative error of at most 0.0022.
Values may be sent and summed in bfloat16 or wider, within the bound.
A program may use at most 128 MiB of HBM per device.

```python
import math
import jax
import jax.numpy as jnp
from jax import lax

D = 2048
HEADS = 32
KEYHEADS = 16
DK = 128
DV = 128
VOCAB = 131072
STEPS = 4
BATCH = 128


def place_ends(result, stream_key, smallest, top_value):
    shape = result.shape
    place = [jax.random.randint(jax.random.fold_in(stream_key, axis), (), 0, shape[axis]) for axis in range(len(shape))]
    result = result.at[tuple(place)].set(smallest)
    longest = shape.index(max(shape))
    place[longest] = (place[longest] + 1) % shape[longest]
    return result.at[tuple(place)].set(top_value)


def shard_levels(own_key, shape, cuts, least, top_value):
    level, own = 1.0, jax.random.fold_in(own_key, 6)
    for axis_at, parts in cuts:
        draws = jnp.exp(jax.random.uniform(jax.random.fold_in(own, axis_at), (parts,), jnp.float32, least / len(cuts), top_value / len(cuts)))
        level = level * jnp.repeat(draws, shape[axis_at] // parts).reshape([-1 if axis == axis_at else 1 for axis in range(len(shape))])
    return level


def bell_draw(key, dims, spread, limit, split=(), kind=jnp.bfloat16):
    drawn = jax.random.normal(key, dims, jnp.float32) * spread
    if len(split) > 0:
        drawn = shard_levels(key, dims, split, -0.22, 0.18) * drawn
    return jnp.clip(drawn, min=-limit, max=limit).astype(kind)


def setup_inputs(seed: int = 0) -> dict:
    streams_of = jax.random.split(jax.random.key(seed), 18)
    return {
        "embedded": bell_draw(streams_of[0], (STEPS, BATCH, D), 1.0, 6.0, ((1, 8),)),
        "states": bell_draw(streams_of[1], (BATCH, HEADS, DK, DV), 0.5, 6.0, ((0, 8), (1, 4))),
        "w_query": bell_draw(streams_of[2], (D, KEYHEADS * DK), D ** -0.5, 0.125, ((1, 4),)),
        "w_key": bell_draw(streams_of[3], (D, KEYHEADS * DK), D ** -0.5, 0.125, ((1, 4),)),
        "w_value": bell_draw(streams_of[4], (D, HEADS * DV), D ** -0.5, 0.125, ((1, 4),)),
        "w_output_gate": bell_draw(streams_of[5], (D, HEADS * DV), D ** -0.5, 0.125, ((1, 4),)),
        "w_beta": bell_draw(streams_of[6], (D, HEADS), D ** -0.5, 0.125, ((1, 4),)),
        "w_decay": bell_draw(streams_of[7], (D, HEADS), D ** -0.5, 0.125, ((1, 4),)),
        "decay_rate": jnp.clip(jnp.exp(jax.random.uniform(streams_of[8], (HEADS,), jnp.float32, math.log(0.05), math.log(4.0))), 0.05, 4.0),
        "decay_bias": jnp.clip(jax.random.uniform(streams_of[9], (HEADS,), jnp.float32, -3.0, 1.0), -3.0, 1.0),
        "head_gain": jnp.clip(1.0 + 0.1 * jax.random.normal(streams_of[10], (DV,), jnp.float32), 0.5, 1.5),
        "input_gain": jnp.clip(1.0 + 0.1 * jax.random.normal(streams_of[11], (D,), jnp.float32), 0.5, 1.5),
        "w_out": bell_draw(streams_of[12], (HEADS * DV, D), (HEADS * DV) ** -0.5, 0.09375, ((0, 4),)),
        "final_gain": jnp.clip(1.0 + 0.1 * jax.random.normal(streams_of[13], (D,), jnp.float32), 0.5, 1.5),
        "lm_head": bell_draw(streams_of[14], (D, VOCAB), 0.066, 1.0, ((1, 32),)),
        "targets": place_ends(jax.random.randint(streams_of[15], (BATCH, STEPS), 0, VOCAB), jax.random.fold_in(streams_of[15], 1), 0, VOCAB - 1).astype(jnp.int32),
        "active": place_ends((jax.random.randint(streams_of[16], (BATCH, STEPS), 0, 4) < 3).astype(jnp.int32), jax.random.fold_in(streams_of[16], 1), 0, 1),
    }


EPS = 1e-06

def rms_scale(values, gain):
    values = values.astype(jnp.float32)
    return values * lax.rsqrt(lax.optimization_barrier(jnp.mean(values * values, axis=-1, keepdims=True)) + EPS) * gain.astype(jnp.float32)

def unit_rows(values):
    return values * lax.rsqrt(lax.optimization_barrier(jnp.sum(values * values, axis=-1, keepdims=True)) + EPS)

def gated_rms_norm(state_readout, gate, head_gain):
    normed = state_readout * lax.rsqrt(lax.optimization_barrier(jnp.mean(state_readout * state_readout, axis=-1, keepdims=True)) + EPS) * head_gain.astype(jnp.float32)
    gate_f = gate.astype(jnp.float32).reshape(state_readout.shape)
    return (normed * jax.nn.silu(gate_f)).astype(jnp.bfloat16)

def one_request(item):
    state, queries, keys, values, betas, decays, marks = item
    state = state.astype(jnp.float32)

    def advance(state, inputs):
        query_vector, key, value, beta, decay, mark = inputs
        decayed_state = state * decay[:, None, None]
        retrieved_value = jnp.einsum('eg,egr->er', key, decayed_state, precision=lax.Precision.HIGHEST)
        update = beta[:, None] * (value - retrieved_value)
        corrected_state = decayed_state + key[:, :, None] * update[:, None, :]
        state_readout = jnp.einsum('eg,egr->er', query_vector, corrected_state, precision=lax.Precision.HIGHEST)
        kept = jnp.where(mark > 0, corrected_state, state)
        return (kept, state_readout)
    _, outs = lax.scan(advance, state, (queries, keys, values, betas, decays, marks))
    return outs

def reference(embedded, states, w_query, w_key, w_value, w_output_gate, w_beta, w_decay, decay_rate, decay_bias, head_gain, input_gain, w_out, final_gain, lm_head, targets, active):
    steps, batch, width = embedded.shape
    normed = rms_scale(embedded, input_gain).astype(jnp.bfloat16).reshape(steps * batch, width)

    def apply_projection(weight):
        return jnp.dot(normed, weight, preferred_element_type=jnp.float32).astype(jnp.bfloat16).reshape(steps, batch, -1)
    query_vector = apply_projection(w_query).astype(jnp.float32).reshape(steps, batch, KEYHEADS, DK)
    key = apply_projection(w_key).astype(jnp.float32).reshape(steps, batch, KEYHEADS, DK)
    value = apply_projection(w_value).astype(jnp.float32).reshape(steps, batch, HEADS, DV)
    gate = apply_projection(w_output_gate)
    beta_raw = apply_projection(w_beta).astype(jnp.float32)
    decay_raw = apply_projection(w_decay).astype(jnp.float32)
    query_vector = jnp.repeat(unit_rows(query_vector) * DK ** (-0.5), 2, axis=2)
    key = jnp.repeat(unit_rows(key), 2, axis=2)
    beta = jax.nn.sigmoid(beta_raw)
    decay = jnp.exp(-decay_rate * jax.nn.softplus(decay_raw + decay_bias))
    marks = active.T
    readouts = lax.map(one_request, (states, jnp.moveaxis(query_vector, 0, 1), jnp.moveaxis(key, 0, 1), jnp.moveaxis(value, 0, 1), jnp.moveaxis(beta, 0, 1), jnp.moveaxis(decay, 0, 1), active))
    readouts = jnp.moveaxis(readouts, 0, 1)
    mixed = gated_rms_norm(readouts, gate, head_gain).reshape(steps * batch, HEADS * DV)
    summed = jnp.dot(mixed, w_out, preferred_element_type=jnp.float32).reshape(steps, batch, width)
    hidden = rms_scale(embedded.astype(jnp.float32) + summed, final_gain).astype(jnp.bfloat16)
    columns = jnp.arange(VOCAB, dtype=jnp.int32)

    def score_step(item):
        rows, target, mark = item
        logits = jnp.dot(rows, lm_head, preferred_element_type=jnp.float32)
        total = lax.optimization_barrier(jnp.sum(jnp.exp(logits), axis=1))
        picked = lax.optimization_barrier(jnp.sum(jnp.where(columns[None, :] == target[:, None], logits, 0.0), axis=1))
        return jnp.where(mark > 0, picked - jnp.log(total), 0.0)
    scores = lax.map(score_step, (hidden, targets.T, marks))
    return scores.T
```

```python
import functools

import jax
import jax.numpy as jnp
from jax import lax
from jax.experimental import pallas as pl
from jax.experimental.pallas import tpu as pltpu
from jax.sharding import PartitionSpec as P

EPS = 1e-06
MESH = pl.DeviceIdType.MESH
F32 = jnp.float32
BF16 = jnp.bfloat16


def pick_lane(values, index):
    lanes = lax.broadcasted_iota(jnp.int32, values.shape, 1)
    return jnp.sum(jnp.where(lanes == index, values, 0.0), axis=1, keepdims=True)


def dot_t(a, b):
    return lax.dot_general(a, b, (((1,), (1,)), ((), ())), preferred_element_type=F32)


def layer_kernel(
    steps, group, local_heads,
    x_ref, gain_ref, wq_ref, wk_ref, wv_ref, wg_ref, wb_ref, wd_ref,
    rate_ref, bias_ref, hgain_ref, active_ref, state_ref, wo_ref,
    out_ref,
    normed, beta_all, decay_all, vecs, prods, mixed, acc,
):
    j = pl.program_id(0)
    head_index = lax.axis_index("head")
    dk = wq_ref.shape[1]

    @pl.when(j == 0)
    def _():
        x = x_ref[...].astype(F32)
        n = x * lax.rsqrt(jnp.mean(x * x, axis=-1, keepdims=True) + EPS) * gain_ref[...]
        n = n.astype(BF16)
        normed[...] = n
        beta_all[...] = dot_t(n, wb_ref[...]).astype(BF16).astype(F32)
        decay_all[...] = dot_t(n, wd_ref[...]).astype(BF16).astype(F32)
        acc[...] = jnp.zeros_like(acc)

    n = normed[...]
    q = jnp.dot(n, wq_ref[...], preferred_element_type=F32).astype(BF16).astype(F32)
    k = jnp.dot(n, wk_ref[...], preferred_element_type=F32).astype(BF16).astype(F32)
    v = jnp.dot(n, wv_ref[...], preferred_element_type=F32).astype(BF16).astype(F32)
    g = jnp.dot(n, wg_ref[...], preferred_element_type=F32).astype(BF16).astype(F32)
    qn = lax.rsqrt(jnp.sum(q * q, axis=-1, keepdims=True) + EPS) * dk ** (-0.5)
    kn = lax.rsqrt(jnp.sum(k * k, axis=-1, keepdims=True) + EPS)
    ks = [k[t * group:(t + 1) * group] for t in range(steps)]
    qs = [q[t * group:(t + 1) * group] for t in range(steps)]
    kns = [kn[t * group:(t + 1) * group] for t in range(steps)]
    qns = [qn[t * group:(t + 1) * group] for t in range(steps)]
    kinds = 2 * steps
    for t in range(steps):
        vecs[pl.ds(t, group, stride=kinds), :] = ks[t]
        vecs[pl.ds(steps + t, group, stride=kinds), :] = qs[t]
    for r in range(group):
        left = vecs[r * kinds:(r + 1) * kinds, :].astype(BF16)
        for h in range(2):
            prods[h, r * kinds:(r + 1) * kinds, :] = jnp.dot(
                left, state_ref[r, h], preferred_element_type=F32
            )

    def gram(a, b):
        return jnp.sum(a * b, axis=-1, keepdims=True)

    kk = {(s, t): gram(ks[s], ks[t]) * kns[s] * kns[t] for t in range(steps) for s in range(t)}
    kq = {(s, t): gram(ks[s], qs[t]) * kns[s] * qns[t] for t in range(steps) for s in range(t + 1)}
    b_index = lax.axis_index("batch")
    act = active_ref[...].astype(F32)
    lanes = lax.broadcasted_iota(jnp.int32, (group, act.shape[1]), 1)
    mine = lanes == b_index * group + lax.broadcasted_iota(jnp.int32, (group, act.shape[1]), 0)
    marks = [
        jnp.sum(jnp.where(mine, act[t:t + 1], 0.0), axis=1, keepdims=True) > 0
        for t in range(steps)
    ]
    hgain = hgain_ref[...]
    for h in range(2):
        local = 2 * j + h
        rate = pick_lane(rate_ref[...], head_index * local_heads + local)
        bias = pick_lane(bias_ref[...], head_index * local_heads + local)
        beta = jax.nn.sigmoid(pick_lane(beta_all[...], local))
        z = pick_lane(decay_all[...], local) + bias
        softplus = jnp.maximum(z, 0.0) + jnp.log1p(jnp.exp(-jnp.abs(z)))
        decay = jnp.exp(-rate * softplus)
        dv = v.shape[1] // 2
        scale = jnp.ones((group, 1), F32)
        weights = []
        updates = []
        for t in range(steps):
            rows = slice(t * group, (t + 1) * group)
            d = decay[rows]
            sk = prods[h, pl.ds(t, group, stride=kinds), :] * (kns[t] * scale)
            sq = prods[h, pl.ds(steps + t, group, stride=kinds), :] * (qns[t] * scale)
            for s in range(t):
                sk = sk + (weights[s] * kk[(s, t)]) * updates[s]
                sq = sq + (weights[s] * kq[(s, t)]) * updates[s]
            u = beta[rows] * (v[rows, h * dv:(h + 1) * dv] - d * sk)
            readout = d * sq + kq[(t, t)] * u
            scale = jnp.where(marks[t], d * scale, scale)
            weights = [jnp.where(marks[t], d * w, w) for w in weights]
            weights.append(jnp.where(marks[t], 1.0, jnp.zeros((group, 1), F32)))
            updates.append(u)
            gate = g[rows, h * dv:(h + 1) * dv]
            m = readout * lax.rsqrt(jnp.mean(readout * readout, axis=-1, keepdims=True) + EPS) * hgain
            mixed[rows, h * dv:(h + 1) * dv] = (m * (gate * jax.nn.sigmoid(gate))).astype(BF16)
    acc[...] += jnp.dot(mixed[...], wo_ref[...], preferred_element_type=F32)

    @pl.when(j == pl.num_programs(0) - 1)
    def _():
        out_ref[...] = acc[...].astype(BF16)


def layer(x, gain, wq, wk, wv, wg, wb, wd, rate, bias, hgain, active, states, wo, steps):
    rows, width = x.shape
    group = rows // steps
    local_heads = wb.shape[0]
    key_heads = local_heads // 2
    dk, dv = states.shape[2], states.shape[3]
    whole = lambda a: pl.BlockSpec(a.shape, lambda j: (0,) * a.ndim)
    return pl.pallas_call(
        functools.partial(layer_kernel, steps, group, local_heads),
        grid=(key_heads,),
        out_shape=jax.ShapeDtypeStruct((rows, width), BF16),
        in_specs=[
            whole(x), whole(gain),
            pl.BlockSpec((width, dk), lambda j: (0, j)),
            pl.BlockSpec((width, dk), lambda j: (0, j)),
            pl.BlockSpec((width, 2 * dv), lambda j: (0, j)),
            pl.BlockSpec((width, 2 * dv), lambda j: (0, j)),
            whole(wb), whole(wd), whole(rate), whole(bias), whole(hgain), whole(active),
            pl.BlockSpec((group, 2, dk, dv), lambda j: (0, j, 0, 0)),
            pl.BlockSpec((2 * dv, width), lambda j: (j, 0)),
        ],
        out_specs=pl.BlockSpec((rows, width), lambda j: (0, 0)),
        scratch_shapes=[
            pltpu.VMEM((rows, width), BF16),
            pltpu.VMEM((rows, local_heads), F32),
            pltpu.VMEM((rows, local_heads), F32),
            pltpu.VMEM((2 * rows, dk), F32),
            pltpu.VMEM((2, 2 * rows, dv), F32),
            pltpu.VMEM((rows, 2 * dv), BF16),
            pltpu.VMEM((rows, width), F32),
        ],
        compiler_params=pltpu.CompilerParams(
            dimension_semantics=("arbitrary",), vmem_limit_bytes=67043328
        ),
        name="layer",
    )(x, gain, wq, wk, wv, wg, wb, wd, rate, bias, hgain, active, states, wo)


def score_kernel(
    nh, nb, tile,
    part_ref, x_ref, gain_ref, targets_ref, lm_ref,
    out_ref,
    lm, got, gathered, stats, arrived,
    lm_sem, rs_send, rs_recv, x_send, x_recv, y_send, y_recv, r_send, r_recv, l_send, l_recv, c_send, c_recv,
    s_send, s_recv,
):
    head = lax.axis_index("head")
    batch = lax.axis_index("batch")
    n = nh * nb
    me = head * nb + batch
    nx, nz = nh // 2, nb // 2
    xi, core = head // 2, head % 2
    zi, yi = batch // 2, batch % 2
    rows = part_ref.shape[0]
    chunk = rows // nh
    half = nx * chunk
    block = 2 * half
    tiles = lm_ref.shape[1] // tile
    cols = lm_ref.shape[1]

    loads = [
        pltpu.make_async_copy(lm_ref.at[:, pl.ds(i * tile, tile)], lm.at[i], lm_sem.at[i])
        for i in range(tiles)
    ]
    for load in loads:
        load.start()

    barrier = pltpu.get_barrier_semaphore()

    def greet(i, carry):
        f = lax.rem(me + i, n)
        pl.semaphore_signal(barrier, inc=1, device_id=(f // nb, f % nb), device_id_type=MESH)
        return carry

    lax.fori_loop(1, n, greet, 0)
    pl.semaphore_wait(barrier, n - 1)

    def remote(src, dst, send, recv, h, b):
        return pltpu.make_async_remote_copy(
            src_ref=src, dst_ref=dst, send_sem=send, recv_sem=recv,
            device_id=(h, b), device_id_type=MESH,
        )

    copies = []
    for i in range(1, nh):
        to = lax.rem(head + i, nh)
        copies.append(remote(
            part_ref.at[pl.ds(pl.multiple_of(to * chunk, chunk), chunk), :], got.at[i],
            rs_send.at[i], rs_recv.at[i], to, batch,
        ))
        copies[-1].start()
    own = pl.ds(pl.multiple_of(head * chunk, chunk), chunk)
    y = part_ref[own, :].astype(F32)
    for i, c in enumerate(copies):
        c.wait()
        y = y + got[i + 1].astype(F32)
    y = y + x_ref[own, :].astype(F32)
    hidden = y * lax.rsqrt(jnp.mean(y * y, axis=-1, keepdims=True) + EPS) * gain_ref[...]

    def slab(x_at):
        return pl.ds(pl.multiple_of(yi * half + x_at * chunk, chunk), chunk)

    gathered[core, zi, slab(xi), :] = hidden.astype(BF16)
    copies = []
    for i in range(1, nx):
        mine = gathered.at[core, zi, slab(xi), :]
        copies.append(remote(
            mine, mine, x_send.at[i], x_recv.at[i], lax.rem(xi + i, nx) * 2 + core, batch))
        copies[-1].start()
    for c in copies:
        c.wait()
    mine = gathered.at[core, zi, pl.ds(pl.multiple_of(yi * half, half), half), :]
    c = remote(mine, mine, y_send, y_recv, head, zi * 2 + (1 - yi))
    c.start()
    c.wait()

    def whole(z_at):
        return gathered.at[core, z_at]

    def right(hop):
        ref = whole(lax.rem(zi - hop + nz, nz))
        return remote(ref, ref, r_send.at[hop], r_recv.at[hop], head, lax.rem(zi + 1, nz) * 2 + yi)

    def left(hop):
        ref = whole(lax.rem(zi + hop, nz))
        return remote(ref, ref, l_send.at[hop], l_recv.at[hop], head, lax.rem(zi + nz - 1, nz) * 2 + yi)

    def share(z_at):
        return remote(
            whole(z_at), whole(z_at), c_send.at[z_at], c_recv.at[z_at], head + 1 - 2 * core, batch
        )

    first = me * cols

    def score(z_at):
        for_rows = jnp.concatenate([targets_ref[0, z_at], targets_ref[1, z_at]], axis=0)
        wanted = for_rows - first
        a = jnp.concatenate([gathered[0, z_at], gathered[1, z_at]], axis=0)
        lanes = lax.broadcasted_iota(jnp.int32, (2 * block, tile), 1)

        def step(i, carry):
            total, picked = carry
            logits = jnp.dot(a, lm[i], preferred_element_type=F32)
            e = jnp.exp(logits)
            p = jnp.where(lanes == wanted - i * tile, logits, 0.0)
            for s in range(tile // 128):
                total = total + e[:, s * 128:(s + 1) * 128]
                picked = picked + p[:, s * 128:(s + 1) * 128]
            return total, picked

        zero = jnp.zeros((2 * block, 128), F32)
        total, picked = lax.fori_loop(0, tiles, step, (zero, zero))
        total = jnp.sum(total, axis=1, keepdims=True)
        picked = jnp.sum(picked, axis=1, keepdims=True)
        lane = lax.broadcasted_iota(jnp.int32, (2 * block, 128), 1)
        both = jnp.where(lane == 0, total, jnp.where(lane == 1, picked, 0.0))
        for y_at in range(2):
            piece = jnp.concatenate([
                both[y_at * half:(y_at + 1) * half],
                both[block + y_at * half:block + (y_at + 1) * half],
                jnp.zeros((128 - 2 * half, 128), F32),
            ], axis=0)
            stats[z_at * 2 + y_at] = piece.T[:8]

    @pl.when(zi + 1 < nz)
    def _():
        right(0).start()

    @pl.when(zi > 0)
    def _():
        left(0).start()

    share(zi).start()
    for load in loads:
        load.wait()
    share(zi).wait()
    score(zi)
    for hop in range(1, nz):
        below = lax.rem(zi - hop + nz, nz)
        above = lax.rem(zi + hop, nz)

        @pl.when(zi >= hop)
        def _():
            ref = whole(below)
            remote(ref, ref, r_send.at[hop - 1], r_recv.at[hop - 1], head, batch).wait_recv()

            @pl.when(zi + 1 < nz)
            def _():
                right(hop).start()

            share(below).start()

        @pl.when(zi + hop < nz)
        def _():
            ref = whole(above)
            remote(ref, ref, l_send.at[hop - 1], l_recv.at[hop - 1], head, batch).wait_recv()

            @pl.when(zi > 0)
            def _():
                left(hop).start()

            share(above).start()

        @pl.when(zi >= hop)
        def _():
            share(below).wait()
            score(below)

        @pl.when(zi + hop < nz)
        def _():
            share(above).wait()
            score(above)

    for hop in range(nz):
        @pl.when((zi + 1 < nz) & (zi >= hop))
        def _():
            right(hop).wait_send()

        @pl.when((zi > 0) & (zi + hop < nz))
        def _():
            left(hop).wait_send()

    def stat(i):
        f = lax.rem(me + i, n)
        return remote(stats.at[f % nb], arrived.at[i], s_send.at[i], s_recv.at[i], f // nb, f % nb)

    def begin(i, carry):
        stat(i).start()
        return carry

    lax.fori_loop(1, n, begin, 0)

    def finish(i, carry):
        stat(i).wait()
        return carry + arrived[i]

    summed = lax.fori_loop(1, n, finish, stats[batch])
    out_ref[...] = summed


def score_parts(part, x, gain, targets, lm_head, nh, nb):
    rows, width = part.shape
    cols = lm_head.shape[1]
    tile = min(512, cols)
    chunk = rows // nh
    block = 2 * (nh // 2) * chunk
    nz = nb // 2
    n = nh * nb
    vmem = pl.BlockSpec(memory_space=pltpu.VMEM)
    dma = pltpu.SemaphoreType.DMA
    return pl.pallas_call(
        functools.partial(score_kernel, nh, nb, tile),
        out_shape=jax.ShapeDtypeStruct((8, 128), F32),
        in_specs=[vmem] * 4 + [pl.BlockSpec(memory_space=pl.ANY)],
        out_specs=vmem,
        scratch_shapes=[
            pltpu.VMEM((cols // tile, width, tile), BF16),
            pltpu.VMEM((nh, chunk, width), BF16),
            pltpu.VMEM((2, nz, block, width), BF16),
            pltpu.VMEM((nb, 8, 128), F32),
            pltpu.VMEM((n, 8, 128), F32),
            dma((cols // tile,)),
            dma((nh,)), dma((nh,)),
            dma((nh,)), dma((nh,)),
            dma, dma,
            dma((nb,)), dma((nb,)),
            dma((nb,)), dma((nb,)),
            dma((nb,)), dma((nb,)),
            dma((n,)), dma((n,)),
        ],
        compiler_params=pltpu.CompilerParams(
            collective_id=0, has_side_effects=True, vmem_limit_bytes=48 << 20
        ),
        name="score",
    )(part, x, gain, targets, lm_head)


def per_device(
    embedded, states, w_query, w_key, w_value, w_output_gate, w_beta, w_decay,
    decay_rate, decay_bias, head_gain, input_gain, w_out, final_gain, lm_head, targets, active,
):
    nh, nb = lax.axis_size("head"), lax.axis_size("batch")
    steps, group, width = embedded.shape
    rows = steps * group
    chunk = rows // nh
    x = embedded.reshape(rows, width)
    part = layer(
        x, input_gain[None], w_query, w_key, w_value, w_output_gate, w_beta.T, w_decay.T,
        decay_rate[None], decay_bias[None], head_gain[None], active.T, states, w_out, steps,
    )
    ordered = (
        targets.reshape(nb, group, steps).transpose(0, 2, 1)
        .reshape(nb // 2, 2, nh // 2, 2, chunk).transpose(3, 0, 1, 2, 4)
        .reshape(2, nb // 2, rows, 1)
    )
    stats = score_parts(part, x, final_gain[None], ordered, lm_head, nh, nb)
    scores = stats[1] - jnp.log(stats[0])
    scores = scores[:rows].reshape(2, nh // 2, chunk).transpose(1, 0, 2).reshape(steps, group).T
    marks = lax.dynamic_slice_in_dim(active, lax.axis_index("batch") * group, group, 0)
    return jnp.where(marks > 0, scores, 0.0)


def solution(mesh):
    return jax.shard_map(
        per_device,
        mesh=mesh,
        in_specs=(
            P(None, "batch", None),
            P("batch", "head", None, None),
            P(None, "head"),
            P(None, "head"),
            P(None, "head"),
            P(None, "head"),
            P(None, "head"),
            P(None, "head"),
            P(),
            P(),
            P(),
            P(),
            P("head", None),
            P(),
            P(None, ("head", "batch")),
            P(),
            P(),
        ),
        out_specs=P("batch", None),
        check_vma=False,
    )
```
